32 devices in a mesh: pair: 8 (over y, x, core), aux: 4 (over z).
Axes of the slice: x: 2, y: 2, z: 4, core: 2. Of those that a mesh axis runs over, the one named last changes fastest.
Arguments:
- integrals: float32 [8, 640, 2048], P(None, 'aux', 'pair'), may hold values from -6 to 6
- factor: float32 [2048, 2048], P('aux', 'pair'), may hold values from -1 to 2, as said below
- diag_inverse: float32 [4, 512, 512], P('aux'), may hold values from -1 to 1, as said below
Outputs:
- transformed: float32 [8, 640, 2048], P('pair', None, 'aux')
The draws below stay inside these ranges and needn't reach their ends.
Inputs may be any that keep to these rules, and one draw needn't show every extreme that they name: factor is zero above its diagonal. diag_inverse[j] is the inverse, up to rounding, of the factor's j-th diagonal block of 512 x 512.
All inputs are finite; a program needn't handle non-finite values.
Results may differ from the reference program's by a relative error of at most 0.0001.
Values sent between devices are 32-bit elements; how exact they have to be, the bound alone decides.
A program may use at most 128 MiB of HBM per device.

```python
import math
import jax
import jax.numpy as jnp
from jax import lax

PANEL = 512
VIRT = 640
OCC = 8
WIN = 2048


def factor_parts(key):
    base = jax.random.fold_in(key, 7)
    first, second = jax.random.split(base)
    diagonal = jax.random.uniform(first, (WIN,), jnp.float32, 1.0, 2.0)
    below = jnp.clip(jax.random.normal(second, (WIN, WIN), jnp.float32), -6.0, 6.0)
    below = below * (0.6 / math.sqrt(WIN))
    factor = jnp.tril(below, -1) + jnp.diag(diagonal)
    blocks = jnp.stack([factor[j * PANEL:(j + 1) * PANEL, j * PANEL:(j + 1) * PANEL] for j in range(WIN // PANEL)])
    identity = jnp.broadcast_to(jnp.eye(PANEL, dtype=jnp.float32), blocks.shape)
    inverses = lax.linalg.triangular_solve(blocks, identity, left_side=True, lower=True)
    return (factor, inverses)


def draw_factor(key, part):
    return factor_parts(key)[0]


def draw_diag_inverse(key, part):
    return factor_parts(key)[1]


def shard_levels(own_key, dims, cuts, least, high):
    loudness = 1.0
    for position, shards_of in cuts:
        draws = jax.random.uniform(jax.random.fold_in(jax.random.fold_in(own_key, 6), position), (shards_of,), jnp.float32, least / len(cuts), high / len(cuts))
        loudness = loudness * jnp.repeat(jnp.exp(draws), dims[position] // shards_of).reshape((-1,) + (1,) * (len(dims) - 1 - position))
    return loudness


def gaussian(own_key, extent, width, limit, pieces=(), kind=jnp.bfloat16):
    result = width * jax.random.normal(own_key, extent, jnp.float32)
    if pieces:
        result = result * shard_levels(own_key, extent, pieces, -0.22, 0.18)
    return jnp.clip(result, -limit, limit).astype(kind)


def setup_inputs(seed: int = 0) -> dict:
    streams_of = jax.random.split(jax.random.key(seed), 4)
    integrals = gaussian(streams_of[0], (OCC, VIRT, WIN), 1.0, 6.0, ((1, 4), (2, 8)), jnp.float32)
    factor = draw_factor(jax.random.fold_in(streams_of[3], 71), 0)
    diag_inverse = draw_diag_inverse(jax.random.fold_in(streams_of[3], 71), 0)
    return dict(integrals=integrals, factor=factor, diag_inverse=diag_inverse)


def reference(integrals, factor, diag_inverse):
    pair_rows = integrals.reshape(-1, WIN)
    panel_count = WIN // PANEL
    solved = []
    for step in range(panel_count):
        remain = pair_rows[:, step * PANEL:(step + 1) * PANEL]
        if step > 0:
            earlier = jnp.concatenate(solved, axis=1)
            factor_block = factor[step * PANEL:(step + 1) * PANEL, :step * PANEL]
            remain = remain - jnp.dot(earlier.astype(jnp.float32), factor_block.T.astype(jnp.float32), precision=lax.Precision.HIGHEST, preferred_element_type=jnp.float32)
        solved.append(jnp.dot(remain.astype(jnp.float32), diag_inverse[step].T.astype(jnp.float32), precision=lax.Precision.HIGHEST, preferred_element_type=jnp.float32))
    return jnp.concatenate(solved, axis=1).reshape(OCC, VIRT, WIN)
```

```python
import functools

import jax
import jax.numpy as jnp
from jax import lax
from jax.experimental import pallas as pl
from jax.experimental.pallas import tpu as pltpu
from jax.sharding import PartitionSpec as P

MESH = pl.DeviceIdType.MESH


def flip(index, mask):
    result = index
    bit = 1
    while bit <= mask:
        if mask & bit:
            result = result + bit * (1 - 2 * ((index // bit) % 2))
        bit *= 2
    return result


def subsets(bits):
    found = [0]
    for bit in bits:
        found = found + [m | bit for m in found]
    return found


def halves_of(value):
    high = value.astype(jnp.bfloat16)
    low = (value - high.astype(jnp.float32)).astype(jnp.bfloat16)
    return high, low


def dot_t(left, right):
    return lax.dot_general(left, right, (((1,), (1,)), ((), ())), preferred_element_type=jnp.float32)


def product(left, right):
    return dot_t(left[0], right[0]) + (dot_t(left[0], right[1]) + dot_t(left[1], right[0]))


def kernel(pairs, panels, integrals, own, out, rows_in, weights, solved, high, low, total,
           own_sem, act_send, act_recv, z_send, z_recv, w_send, w_recv, out_send, out_recv):
    p = lax.axis_index("pair")
    z = lax.axis_index("aux")
    each = pairs // panels
    width, cols = own.shape
    occ = rows_in.shape[1]
    virt = rows_in.shape[2]
    rows = occ * virt
    half = width // 2
    bits = [1 << b for b in range(1, pairs.bit_length() - 1)]
    orders = (bits, bits[::-1])
    stages = len(bits)

    def low_of(j):
        return pairs - each if j == 0 else 0

    def base(j):
        return each * (j * (j + 1) // 2)

    def held(j, q):
        return jnp.logical_and(q >= low_of(j), q < low_of(j) + (j + 1) * each)

    def slot(j, q):
        return base(j) + q - low_of(j)

    def on(condition, action):
        pl.when(condition)(action)

    barrier = pltpu.get_barrier_semaphore()
    for m in range(1, pairs):
        pl.semaphore_signal(barrier, inc=1, device_id={"pair": flip(p, m)}, device_id_type=MESH)
    for d in range(1, panels):
        pl.semaphore_signal(barrier, inc=1, device_id={"aux": (z + d) % panels}, device_id_type=MESH)

    def own_copy(j):
        return pltpu.make_async_copy(own, weights.at[slot(j, p)], own_sem.at[0])

    own_rows = pltpu.make_async_copy(integrals.at[pl.ds(p * occ, occ)], rows_in.at[p], own_sem.at[1])
    own_rows.start()
    for j in range(panels):
        on(jnp.logical_and(z == j, held(j, p)), lambda j=j: own_copy(j).start())
    for j in range(panels):
        on(jnp.logical_and(z == j, held(j, p)), lambda j=j: own_copy(j).wait())
    pl.semaphore_wait(barrier, pairs - 1 + panels - 1)

    def z_copy(j, way):
        ref = weights.at[slot(j, p)]
        step = 1 if way else -1
        return pltpu.make_async_remote_copy(
            ref, ref, z_send.at[j, way], z_recv.at[j], device_id={"aux": z + step}, device_id_type=MESH)

    def z_sends(j, way, source):
        edge = z < panels - 1 if way else z > 0
        side = z == j if source else (z > j if way else z < j)
        return jnp.logical_and(jnp.logical_and(edge, side), held(j, p))

    for j in range(panels):
        for way in range(2):
            on(z_sends(j, way, True), lambda j=j, way=way: z_copy(j, way).start())

    def act_copy(m):
        target = flip(p, m)
        return pltpu.make_async_remote_copy(
            integrals.at[pl.ds(target * occ, occ)], rows_in.at[p], act_send.at[m], act_recv.at[m],
            device_id={"pair": target}, device_id_type=MESH)

    for m in range(1, pairs):
        act_copy(m).start()

    def w_copy(j, h, rel, bit):
        ref = weights.at[slot(j, flip(p, rel ^ bit)), pl.ds(h * half, half)]
        return pltpu.make_async_remote_copy(
            ref, ref, w_send.at[j, h, rel], w_recv.at[j, h, rel],
            device_id={"pair": flip(p, bit)}, device_id_type=MESH)

    sent = []

    def w_start(j, h, m, bit):
        on(held(j, flip(p, m)), lambda: w_copy(j, h, m ^ bit, bit).start())
        sent.append((j, h, m, bit))

    def w_wait(j, h, rel):
        ref = weights.at[slot(j, flip(p, rel)), pl.ds(h * half, half)]

        def wait():
            pltpu.make_async_remote_copy(
                ref, ref, w_send.at[j, h, rel], w_recv.at[j, h, rel],
                device_id={"pair": flip(p, 1)}, device_id_type=MESH).wait_recv()

        on(held(j, flip(p, rel)), wait)

    def stage(j, s):
        for h in range(2):
            for m in subsets(orders[h][:s]):
                w_start(j, h, m, orders[h][s])

    def stage_wait(j, s):
        for h in range(2):
            for m in subsets(orders[h][:s]):
                w_wait(j, h, m ^ orders[h][s])
                w_start(j, h, m ^ orders[h][s], 1)

    for j in range(panels):
        on(jnp.logical_and(z != j, held(j, p)), lambda j=j: z_copy(j, 0).wait_recv())
        for way in range(2):
            on(z_sends(j, way, False), lambda j=j, way=way: z_copy(j, way).start())
        stage(j, 0)
        for h in range(2):
            w_start(j, h, 0, 1)

    own_rows.wait()
    for m in range(1, pairs):
        act_copy(m).wait_recv()

    def out_copy(j):
        return pltpu.make_async_remote_copy(
            solved.at[j], out.at[:, pl.ds(pl.multiple_of(z * virt, 8), virt)], out_send.at[j], out_recv.at[z],
            device_id={"aux": j}, device_id_type=MESH)

    def keep_copy(j):
        return pltpu.make_async_copy(
            solved.at[j], out.at[:, pl.ds(pl.multiple_of(z * virt, 8), virt)], out_send.at[j])

    def solve(j):
        if j:
            total[...] = jnp.zeros_like(total)

            def add(q, carry):
                total[...] += product((high[q], low[q]), halves_of(weights[base(j) + q]))
                return carry

            lax.fori_loop(0, j * each, add, 0)
        answer = None
        for t in range(each):
            remain = rows_in[j * each + t].reshape(rows, cols)
            if j:
                remain = remain - total[:, t * cols:(t + 1) * cols]
            term = product(halves_of(remain), halves_of(weights[base(j) + j * each + t]))
            answer = term if answer is None else answer + term
        solved[j] = answer.reshape(occ, virt, width)
        if j + 1 < panels:
            for t in range(each):
                high_t, low_t = halves_of(answer[:, t * cols:(t + 1) * cols])
                high[j * each + t] = high_t
                low[j * each + t] = low_t
        on(z != j, lambda: out_copy(j).start())
        on(z == j, lambda: keep_copy(j).start())

    for j in range(panels + 1):
        if j < panels:
            for s in range(1, stages):
                stage_wait(j, s - 1)
                stage(j, s)
        if j:
            stage_wait(j - 1, stages - 1)
            for h in range(2):
                for m in subsets(bits):
                    w_wait(j - 1, h, m ^ 1)
            solve(j - 1)

    for m in range(1, pairs):
        act_copy(m).wait_send()
    for j in range(panels):
        for way in range(2):
            on(jnp.logical_or(z_sends(j, way, True), z_sends(j, way, False)),
               lambda j=j, way=way: z_copy(j, way).wait_send())
    for j, h, m, bit in sent:
        on(held(j, flip(p, m)), lambda j=j, h=h, m=m, bit=bit: w_copy(j, h, m ^ bit, bit).wait_send())
    for j in range(panels):
        on(z == j, lambda j=j: keep_copy(j).wait())
        on(z != j, lambda j=j: out_copy(j).wait_send())

    def out_wait(source):
        pltpu.make_async_remote_copy(
            solved.at[0], out.at[:, pl.ds(source * virt, virt)], out_send.at[0], out_recv.at[source],
            device_id={"aux": (z + 1) % panels}, device_id_type=MESH).wait_recv()

    for source in range(panels):
        on(z != source, lambda source=source: out_wait(source))


def local(integrals, factor, diag_inverse):
    pairs = lax.axis_size("pair")
    panels = lax.axis_size("aux")
    p = lax.axis_index("pair")
    z = lax.axis_index("aux")
    width, cols = factor.shape
    occ_all, virt, _ = integrals.shape
    each = pairs // panels
    occ = occ_all // pairs
    t = jnp.where(z == 0, p - (pairs - each), p - z * each)
    inside = jnp.logical_and(t >= 0, t < each)
    own_diag = lax.dynamic_slice(diag_inverse[0], (0, jnp.clip(t, 0, each - 1) * cols), (width, cols))
    own = jnp.where(inside, own_diag, factor)
    vmem = pl.BlockSpec(memory_space=pltpu.VMEM)
    dma = pltpu.SemaphoreType.DMA
    blocks = each * panels * (panels + 1) // 2
    return pl.pallas_call(
        functools.partial(kernel, pairs, panels),
        out_shape=jax.ShapeDtypeStruct((occ, virt * panels, width), jnp.float32),
        in_specs=[vmem, vmem],
        out_specs=vmem,
        scratch_shapes=[
            pltpu.VMEM((pairs, occ, virt, cols), jnp.float32),
            pltpu.VMEM((blocks, width, cols), jnp.float32),
            pltpu.VMEM((panels, occ, virt, width), jnp.float32),
            pltpu.VMEM((pairs, occ * virt, cols), jnp.bfloat16),
            pltpu.VMEM((pairs, occ * virt, cols), jnp.bfloat16),
            pltpu.VMEM((occ * virt, width), jnp.float32),
            dma((2,)),
            dma((pairs,)),
            dma((pairs,)),
            dma((panels, 2)),
            dma((panels,)),
            dma((panels, 2, pairs)),
            dma((panels, 2, pairs)),
            dma((panels,)),
            dma((panels,)),
        ],
        compiler_params=pltpu.CompilerParams(
            collective_id=0, has_side_effects=True, vmem_limit_bytes=60 * 1024 * 1024),
    )(integrals, own)


def solution(mesh):
    in_specs = (P(None, "aux", "pair"), P("aux", "pair"), P("aux", None, None))
    out_specs = P("pair", None, "aux")
    return jax.shard_map(local, mesh=mesh, in_specs=in_specs, out_specs=out_specs, check_vma=False)
```
